32 devices in a mesh: seq: 8 (over y, x, core), head: 4 (over z).
Axes of the slice: x: 2, y: 2, z: 4, core: 2. Of those that a mesh axis runs over, the one named last changes fastest.
Arguments:
- queries: bfloat16 [1536, 4096], P('seq', 'head'), may hold values from -1024 to 1024
- image_keys: bfloat16 [12808, 512], P('seq', 'head'), may hold values from -8 to 8
- image_values: bfloat16 [12808, 512], P('seq', 'head'), may hold values from -6 to 6
- layer_input: bfloat16 [1536, 8192], P('seq', 'head'), may hold values from -6 to 6
- out_weight: bfloat16 [4096, 8192], P('head'), may hold values from -0.125 to 0.125
- tile_counts: int32 [4], replicated, may hold values from 1 to 4, as said below
- image_range: int32 [2, 1536], P(None, 'seq'), may hold values from 0 to 4, as said below
- attn_gate: float32 [1], replicated, may hold values from 0.5 to 1.5
Outputs:
- layer_out: bfloat16 [1536, 8192], P('seq', 'head')
The draws below stay inside these ranges and needn't reach their ends.
Inputs may be any that keep to these rules, and one draw needn't show every extreme that they name: `tile_counts`: each image has 1 to 4 tiles and together they have 8; some image has exactly 4. Images are numbered in text order. For every token t, image_range[0, t] <= image_range[1, t]; image_range[1, t] never decreases as t grows; image_range[1, 0] = 0, so tokens before the first image attend to none.
All inputs are finite; a program needn't handle non-finite values.
Results may differ from the reference program's by a relative error of at most 0.0055.
Values may be sent and summed in bfloat16 or wider, within the bound.
A program may use at most 512 MiB of HBM per device.

```python
import math
import jax
import jax.numpy as jnp
from jax import lax

D = 8192
HD = 128
GROUP = 8
TILE_TOK = 1601
TOK_DEV = 192
KVH = 4
HQ = 32
TEXT = 1536
TILES = 8
IMAGES = 4
IMG_TOK = 12808
N_SEQ = 8


def tile_plan(key):
    biggest = jax.random.randint(jax.random.fold_in(key, 31), (), 0, IMAGES)
    extra = TILES - IMAGES - 3
    slots = jax.random.permutation(jax.random.fold_in(key, 32), (IMAGES - 1) * 3)[:extra]
    others = 1 + jnp.sum((slots[None, :] // 3 == jnp.arange(IMAGES - 1, dtype=jnp.int32)[:, None]).astype(jnp.int32), axis=1)
    index = jnp.arange(IMAGES, dtype=jnp.int32)
    ranked = jnp.clip(index - (index > biggest).astype(jnp.int32), 0, IMAGES - 2)
    picked = jnp.sum(jnp.where(ranked[:, None] == jnp.arange(IMAGES - 1, dtype=jnp.int32)[None, :], others[None, :], 0), axis=1)
    return jnp.where(index == biggest, 4, picked).astype(jnp.int32)


def range_plan(key):
    picks = jax.random.permutation(jax.random.fold_in(key, 11), TEXT - 1)[:IMAGES] + 1
    starts = jnp.sort(picks).astype(jnp.int32)
    position = jnp.arange(TEXT, dtype=jnp.int32)
    high = jnp.sum((starts[None, :] <= position[:, None]).astype(jnp.int32), axis=1)
    spread = jax.random.randint(jax.random.fold_in(key, 12), (TEXT,), 0, 1 << 20)
    reach = jnp.maximum(jnp.minimum(high, 3), 1)
    low = jnp.maximum(high - 1 - spread % reach, 0)
    return jnp.stack([low, high]).astype(jnp.int32)


def drawn_pair(key):
    keys = jnp.clip(jax.random.normal(jax.random.fold_in(key, 21), (IMG_TOK, KVH * HD), jnp.float32), -6.0, 6.0)
    queries = jnp.clip(jax.random.normal(jax.random.fold_in(key, 22), (TEXT, HQ * HD), jnp.float32), -6.0, 6.0)
    return (queries, keys)


def draw_queries(key, part):
    return drawn_pair(key)[0].astype(jnp.bfloat16)


def draw_image_keys(key, part):
    return drawn_pair(key)[1].astype(jnp.bfloat16)


def draw_tile_counts(key, part):
    return tile_plan(key)


def draw_image_range(key, part):
    return range_plan(key)


def strengthened(drawn, key, source, target, blocks, factor):
    def block_of(dim):
        return (jnp.arange(drawn.shape[dim]) // (drawn.shape[dim] // blocks)).reshape((-1,) + (1,) * (drawn.ndim - 1 - dim))

    near = jax.random.permutation(key, blocks)[block_of(target)]
    second = (block_of(target) + blocks // 2) % blocks
    return jnp.where((block_of(source) == near) | (block_of(source) == second), factor * drawn, drawn)


def block_scale(rng, extent, cuts, least, high):
    level, own = 1.0, jax.random.fold_in(rng, 6)
    for axis_at, parts in cuts:
        heights = jnp.exp(jax.random.uniform(jax.random.fold_in(own, axis_at), (parts,), jnp.float32, least / len(cuts), high / len(cuts)))
        level = level * jnp.repeat(heights, extent[axis_at] // parts).reshape([-1 if axis == axis_at else 1 for axis in range(len(extent))])
    return level


def scatter_about(key, extent, deviation, bound, split=(), held_as=jnp.bfloat16):
    drawn = deviation * jax.random.normal(key, extent, jnp.float32)
    if split:
        drawn = drawn * block_scale(key, extent, split, -0.22, 0.18)
    return jnp.clip(drawn, -bound, bound).astype(held_as)


def bell_draw_with(key, dims, scale, limit, shards, heavy, kind=jnp.bfloat16):
    array = scale * jax.random.normal(key, dims, jnp.float32)
    if shards:
        array = array * block_scale(key, dims, shards, -0.22, 0.18)
    return jnp.clip(strengthened(array, jax.random.fold_in(key, 3), *heavy), -limit, limit).astype(kind)


def setup_inputs(seed: int = 0) -> dict:
    arg_keys = jax.random.split(jax.random.key(seed), 9)
    return {
        "queries": draw_queries(jax.random.fold_in(arg_keys[8], 71), 0),
        "image_keys": draw_image_keys(jax.random.fold_in(arg_keys[8], 71), 0),
        "image_values": scatter_about(arg_keys[2], (IMG_TOK, KVH * HD), 1.0, 6.0, ((0, 8), (1, 4))),
        "layer_input": scatter_about(arg_keys[3], (TEXT, D), 1.0, 6.0, ((0, 8), (1, 4))),
        "out_weight": bell_draw_with(arg_keys[4], (HQ * HD, D), (HQ * HD) ** -0.5, 0.125, ((0, 4),), (0, 1, 4, 2.0)),
        "tile_counts": draw_tile_counts(jax.random.fold_in(arg_keys[8], 71), 0),
        "image_range": draw_image_range(jax.random.fold_in(arg_keys[8], 71), 0),
        "attn_gate": jnp.clip(jax.random.uniform(arg_keys[7], (1,), jnp.float32, 0.5, 1.5), 0.5, 1.5),
    }


def group_attention(item, key_image, low, high):
    q_group, k_group, v_group = item
    blocks = q_group.reshape(N_SEQ, TOK_DEV, GROUP, HD)
    lows = low.reshape(N_SEQ, TOK_DEV)
    highs = high.reshape(N_SEQ, TOK_DEV)

    def one_block(block_item):
        q_block, low_block, high_block = block_item
        scores = jnp.einsum('tgd,kd->tgk', q_block.astype(jnp.float32), k_group.astype(jnp.float32))
        scores = scores * (1.0 / math.sqrt(HD))
        allowed = (low_block[:, None] <= key_image[None, :]) & (key_image[None, :] < high_block[:, None])
        masked = jnp.where(allowed[:, None, :], scores, -jnp.inf)
        live = high_block > low_block
        top = jnp.where(live[:, None], lax.optimization_barrier(jnp.max(masked, axis=2)), 0.0)
        weights = jnp.exp(masked - top[:, :, None])
        total = lax.optimization_barrier(jnp.sum(weights, axis=2))
        numer = jnp.einsum('tgk,kd->tgd', weights.astype(jnp.bfloat16).astype(jnp.float32), v_group.astype(jnp.float32))
        safe_total = jnp.where(live[:, None], total, 1.0)
        result = jnp.where(live[:, None, None], numer / safe_total[:, :, None], 0.0)
        return result.astype(jnp.bfloat16)
    mapped = lax.map(one_block, (blocks, lows, highs))
    return mapped.reshape(TEXT, GROUP, HD)

def reference(queries, image_keys, image_values, layer_input, out_weight, tile_counts, image_range, attn_gate):
    ends = jnp.cumsum(tile_counts).astype(jnp.int32)
    tile = jnp.arange(IMG_TOK, dtype=jnp.int32) // TILE_TOK
    key_image = lax.optimization_barrier(jnp.sum((ends[None, :] <= tile[:, None]).astype(jnp.int32), axis=1))
    low = image_range[0]
    high = image_range[1]
    q_heads = jnp.transpose(queries.reshape(TEXT, KVH, GROUP, HD), (1, 0, 2, 3))
    k_heads = jnp.transpose(image_keys.reshape(IMG_TOK, KVH, HD), (1, 0, 2))
    v_heads = jnp.transpose(image_values.reshape(IMG_TOK, KVH, HD), (1, 0, 2))
    per_group = lax.map(lambda item: group_attention(item, key_image, low, high), (q_heads, k_heads, v_heads))
    attended = jnp.transpose(per_group, (1, 0, 2, 3)).reshape(TEXT, HQ * HD)
    projected = jnp.dot(attended, out_weight, preferred_element_type=jnp.float32)
    gate = jnp.tanh(attn_gate[0])
    return (layer_input.astype(jnp.float32) + gate * projected).astype(jnp.bfloat16)
```

```python
import functools
import math

import jax
import jax.numpy as jnp
from jax import lax
from jax.experimental import pallas as pl
from jax.experimental.pallas import tpu as pltpu
from jax.sharding import PartitionSpec as P

MESH = pl.DeviceIdType.MESH
NEG = -1e30
BIG = 1e30
LANES = 128
PACK = 16


def round_up(value, unit):
    return -(-value // unit) * unit


def kernel(
    plan,
    counts_ref,
    gate_ref,
    q_ref,
    range_ref,
    k_hbm,
    v_hbm,
    w_hbm,
    x_hbm,
    out_ref,
    kv,
    staged,
    weight,
    residual,
    q_wide,
    bounds,
    scores,
    values,
    run_max,
    numer,
    turned,
    attended,
    term,
    sent,
    from_left,
    from_right,
    own_sem,
    weight_sem,
    residual_sem,
    kv_send,
    kv_recv,
    right_send,
    right_recv,
    left_send,
    left_recv,
):
    devices, heads, tile_rows, split, padded, images, chunks, strip = plan
    square = devices == 8
    chips = devices // 2
    me = lax.axis_index("seq")
    h = lax.axis_index("head")
    core = lax.rem(me, 2)
    chip = me // 2
    partner = chip * 2 + (1 - core)
    rows, width = q_ref.shape
    head_dim = kv.shape[3]
    group = width // head_dim
    strips = group * rows // strip
    columns = out_ref.shape[1]
    halves = ((0, split), (split, padded - split))

    def chip_at(offset):
        if square:
            cy, cx = chip // 2, lax.rem(chip, 2)
            oy, ox = offset // 2, lax.rem(offset, 2)
            return lax.rem(cy + oy, 2) * 2 + lax.rem(cx + ox, 2)
        return lax.rem(chip + offset, chips)

    def at(target):
        return (target, h)

    own = [
        pltpu.make_async_copy(
            source, staged.at[which], own_sem.at[which]
        )
        for which, source in enumerate((k_hbm, v_hbm))
    ]
    for copy in own:
        copy.start()
    fetch = pltpu.make_async_copy(w_hbm, weight, weight_sem)
    fetch.start()
    take = pltpu.make_async_copy(x_hbm, residual, residual_sem)
    take.start()

    barrier = pltpu.get_barrier_semaphore()
    pl.semaphore_signal(barrier, inc=1, device_id=at(partner), device_id_type=MESH)
    for offset in range(1, chips):
        if square and offset == 3:
            continue
        pl.semaphore_signal(
            barrier, inc=1, device_id=at(chip_at(offset) * 2 + core), device_id_type=MESH
        )
    greeted = 1 + (2 if square else chips - 1)

    @pl.when(h > 0)
    def _():
        pl.semaphore_signal(barrier, inc=1, device_id=(me, h - 1), device_id_type=MESH)

    @pl.when(h < heads - 1)
    def _():
        pl.semaphore_signal(barrier, inc=1, device_id=(me, h + 1), device_id_type=MESH)

    ends = jnp.where(h > 0, 1, 0) + jnp.where(h < heads - 1, 1, 0)

    factor = math.log2(math.e) / math.sqrt(head_dim)
    run_max[...] = jnp.full_like(run_max, NEG)
    numer[...] = jnp.zeros_like(numer)
    values[...] = jnp.ones_like(values)
    for g in range(group):
        exact = q_ref[:, g * head_dim : (g + 1) * head_dim].astype(jnp.float32) * factor
        high = exact.astype(jnp.bfloat16)
        part = pl.ds(g * rows, rows)
        q_wide[:head_dim, part] = high.T
        q_wide[head_dim:, part] = (exact - high.astype(jnp.float32)).astype(jnp.bfloat16).T
        bounds[:, part] = range_ref[...]
    whole_rows = tile_rows // PACK * PACK
    for which, copy in enumerate(own):
        copy.wait()
        kv[me, which, :whole_rows, :] = staged[which, :whole_rows, :]
        if whole_rows < padded:
            rest = staged[which, whole_rows:, :]
            kv[me, which, whole_rows:, :] = jnp.concatenate(
                [rest, jnp.zeros((padded - tile_rows, head_dim), rest.dtype)], axis=0
            )
    pl.semaphore_wait(barrier, greeted + ends)

    def kv_copy(slot, half, target, lane):
        start, size = halves[half]
        piece = kv.at[slot, :, pl.ds(start, size), :]
        return pltpu.make_async_remote_copy(
            src_ref=piece,
            dst_ref=piece,
            send_sem=kv_send.at[lane, half],
            recv_sem=kv_recv.at[slot, half],
            device_id=at(target),
            device_id_type=MESH,
        )

    def outgoing(offset, half):
        return kv_copy(me, half, chip_at(offset) * 2 + core, chips + offset)

    def to_partner(offset, half):
        return kv_copy(chip_at(offset) * 2 + core, half, partner, offset)

    def relay(half):
        source = 1 if half == 0 else 2
        return kv_copy(
            chip_at(source) * 2 + core, half, chip_at(3 - source) * 2 + core, chips + 3
        )

    if square:
        outgoing(1, 0).start()
        outgoing(2, 1).start()
        outgoing(1, 1).start()
        outgoing(2, 0).start()
    else:
        for offset in range(1, chips):
            for half in range(2):
                outgoing(offset, half).start()

    to_partner(0, 0).start()
    to_partner(0, 1).start()

    def image_of(slot):
        image, end = 0, 0
        for i in range(images):
            end = end + counts_ref[i]
            image = image + jnp.where(end <= slot, 1, 0)
        return image

    real = tile_rows - split
    edge = real // PACK * PACK

    def attend(slot_a, slot_b):
        image_a, image_b = image_of(slot_a), image_of(slot_b)
        values[:head_dim, :split] = kv[slot_a, 1, :split, :].T
        values[:head_dim, split:] = kv[slot_b, 1, split:, :].T

        def lanes(g):
            return slice(g * strip, (g + 1) * strip)

        def allowed(g, image):
            low, high = bounds[0:1, lanes(g)], bounds[1:2, lanes(g)]
            return (low <= image) & (image < high)

        def score(g):
            q = q_wide[:, lanes(g)]

            def one(keys):
                return jnp.dot(
                    jnp.concatenate([keys, keys], axis=1), q, preferred_element_type=jnp.float32
                )

            s_a = one(kv[slot_a, 0, :split, :])
            s_b = one(kv[slot_b, 0, split:, :])
            row = lax.broadcasted_iota(jnp.int32, s_b[edge:].shape, 0)
            s_b = jnp.concatenate([s_b[:edge], jnp.where(row < real - edge, s_b[edge:], NEG)], axis=0)
            scores[g % 2, :split, :] = s_a
            scores[g % 2, split:, :] = s_b
            return jnp.max(s_a, axis=0, keepdims=True), jnp.max(s_b, axis=0, keepdims=True)

        def mix(g, tops):
            ok_a, ok_b = allowed(g, image_a), allowed(g, image_b)
            old = run_max[g]
            new = jnp.maximum(
                old, jnp.maximum(jnp.where(ok_a, tops[0], NEG), jnp.where(ok_b, tops[1], NEG))
            )
            base_a = jnp.where(ok_a, new, BIG)
            base_b = jnp.where(ok_b, new, BIG)
            p_a = jnp.exp2(scores[g % 2, :split, :] - base_a).astype(jnp.bfloat16)
            p_b = jnp.exp2(scores[g % 2, split:, :] - base_b).astype(jnp.bfloat16)
            run_max[g] = new
            mixed = jnp.dot(
                values[...], jnp.concatenate([p_a, p_b], axis=0), preferred_element_type=jnp.float32
            )
            numer[g] = numer[g] * jnp.exp2(old - new) + mixed

        tops = score(0)
        for g in range(strips):
            later = score(g + 1) if g + 1 < strips else None
            mix(g, tops)
            tops = later

    def turn(step, carry):
        phase = step // 2
        other = lax.rem(step, 2)
        if square:
            off_a = phase
            off_b = jnp.where(phase == 1, 2, jnp.where(phase == 2, 1, phase))
        else:
            off_a = phase
            off_b = phase
        which = jnp.where(other == 0, core, 1 - core)
        slot_a = chip_at(off_a) * 2 + which
        slot_b = chip_at(off_b) * 2 + which

        @pl.when(step > 0)
        def _():
            kv_copy(slot_a, 0, partner, 0).wait_recv()
            kv_copy(slot_b, 1, partner, 0).wait_recv()

        if square:
            @pl.when(step == 2)
            def _():
                relay(0).start()
                relay(1).start()

        @pl.when((other == 0) & (step > 0))
        def _():
            to_partner(off_a, 0).start()
            to_partner(off_b, 1).start()

        attend(slot_a, slot_b)
        return carry

    lax.fori_loop(0, devices, turn, 0)

    for g in range(strips):
        part = slice(g * strip, (g + 1) * strip)
        live = bounds[0:1, part] < bounds[1:2, part]
        whole = numer[g, head_dim : head_dim + 1, :]
        result = jnp.where(live, numer[g, :head_dim, :] / jnp.where(live, whole, 1.0), 0.0)
        turned[part, :] = result.T
    for g in range(group):
        attended[:, g * head_dim : (g + 1) * head_dim] = turned[
            g * rows : (g + 1) * rows, :
        ].astype(jnp.bfloat16)
    fetch.wait()

    piece = 512 if columns % 512 == 0 else columns
    chunk_rows = rows // chunks

    def project(dest):
        def block(j, carry):
            where = pl.ds(pl.multiple_of(dest * columns + j * piece, LANES), piece)
            term[:, where] = jnp.dot(
                attended[...], weight[:, where], preferred_element_type=jnp.float32
            )
            return carry

        lax.fori_loop(0, columns // piece, block, 0)

    def chunk_of(c):
        return pl.ds(pl.multiple_of(c * chunk_rows, chunk_rows), chunk_rows)

    def block_of(dest):
        return pl.ds(pl.multiple_of(dest * columns, LANES), columns)

    def right_copy(i, c):
        return pltpu.make_async_remote_copy(
            src_ref=sent.at[heads - 1 - i, chunk_of(c), :],
            dst_ref=from_left.at[i, chunk_of(c), :],
            send_sem=right_send.at[i, c],
            recv_sem=right_recv.at[i, c],
            device_id=(me, h + 1),
            device_id_type=MESH,
        )

    def left_copy(i, c):
        return pltpu.make_async_remote_copy(
            src_ref=sent.at[i, chunk_of(c), :],
            dst_ref=from_right.at[i, chunk_of(c), :],
            send_sem=left_send.at[i, c],
            recv_sem=left_recv.at[i, c],
            device_id=(me, h - 1),
            device_id_type=MESH,
        )

    def pass_on(dest, i, c, copy, arrived, first):
        @pl.when(first)
        def _():
            sent[dest, chunk_of(c), :] = term[chunk_of(c), block_of(dest)].astype(sent.dtype)

        @pl.when(jnp.logical_not(first))
        def _():
            copy(i, c).wait_recv()
            sent[dest, chunk_of(c), :] = (
                term[chunk_of(c), block_of(dest)]
                + arrived[i, chunk_of(c), :].astype(jnp.float32)
            ).astype(sent.dtype)

        copy(i, c).start()

    def spread(i, carry):
        far = heads - 1 - i

        @pl.when(h < far)
        def _():
            project(far)

        @pl.when(h > i)
        def _():
            project(i)

        def one_chunk(c, inner):
            @pl.when(h < far)
            def _():
                pass_on(far, i, c, right_copy, from_left, h == 0)

            @pl.when(h > i)
            def _():
                pass_on(i, i, c, left_copy, from_right, h == heads - 1)

            return inner

        lax.fori_loop(0, chunks, one_chunk, 0)
        return carry

    lax.fori_loop(0, heads - 1, spread, 0)
    project(h)

    take.wait()
    gate = jnp.tanh(jnp.full((8, LANES), gate_ref[0], jnp.float32))[0:1, 0:1]

    def gather(c, carry):
        @pl.when(h < heads - 1)
        def _():
            left_copy(h, c).wait_recv()
            term[chunk_of(c), block_of(h)] += from_right[h, chunk_of(c), :].astype(jnp.float32)

        @pl.when(h > 0)
        def _():
            right_copy(heads - 1 - h, c).wait_recv()
            term[chunk_of(c), block_of(h)] += from_left[heads - 1 - h, chunk_of(c), :].astype(
                jnp.float32
            )

        out_ref[chunk_of(c), :] = (
            residual[chunk_of(c), :].astype(jnp.float32) + gate * term[chunk_of(c), block_of(h)]
        ).astype(out_ref.dtype)
        return carry

    lax.fori_loop(0, chunks, gather, 0)

    for offset in range(chips):
        for half in range(2):
            to_partner(offset, half).wait_send()
            if square and offset == 3:
                relay(half).wait_send()
            elif offset > 0:
                outgoing(offset, half).wait_send()

    def drain(i, carry):
        def one_chunk(c, inner):
            @pl.when(h < heads - 1 - i)
            def _():
                right_copy(i, c).wait_send()

            @pl.when(h > i)
            def _():
                left_copy(i, c).wait_send()

            return inner

        lax.fori_loop(0, chunks, one_chunk, 0)
        return carry

    lax.fori_loop(0, heads - 1, drain, 0)


def shards(
    queries, image_keys, image_values, layer_input, out_weight, tile_counts, image_range, attn_gate
):
    devices = lax.axis_size("seq")
    heads = lax.axis_size("head")
    rows, width = queries.shape
    tile_rows, head_dim = image_keys.shape
    group = width // head_dim
    columns = layer_input.shape[1]
    padded = round_up(tile_rows, PACK)
    split = max(round_up(padded // 2 - LANES, LANES), LANES)
    chunks = 4 if rows % (4 * PACK) == 0 else 1
    images = tile_counts.shape[0]
    strip = math.gcd(group * rows, 2 * LANES)
    strips = group * rows // strip
    plan = (devices, heads, tile_rows, split, padded, images, chunks, strip)
    low = jnp.bfloat16
    vmem = pl.BlockSpec(memory_space=pltpu.VMEM)
    smem = pl.BlockSpec(memory_space=pltpu.SMEM)
    hbm = pl.BlockSpec(memory_space=pl.ANY)
    hops = max(heads - 1, 1)
    return pl.pallas_call(
        functools.partial(kernel, plan),
        out_shape=jax.ShapeDtypeStruct((rows, columns), low),
        in_specs=[smem, smem, vmem, vmem, hbm, hbm, hbm, hbm],
        out_specs=vmem,
        scratch_shapes=[
            pltpu.VMEM((devices, 2, padded, head_dim), low),
            pltpu.VMEM((2, tile_rows, head_dim), low),
            pltpu.VMEM(out_weight.shape, low),
            pltpu.VMEM((rows, columns), low),
            pltpu.VMEM((2 * head_dim, group * rows), low),
            pltpu.VMEM((2, group * rows), jnp.int32),
            pltpu.VMEM((2, padded, strip), jnp.float32),
            pltpu.VMEM((head_dim + PACK, padded), low),
            pltpu.VMEM((strips, 1, strip), jnp.float32),
            pltpu.VMEM((strips, head_dim + PACK, strip), jnp.float32),
            pltpu.VMEM((group * rows, head_dim), jnp.float32),
            pltpu.VMEM((rows, width), low),
            pltpu.VMEM((rows, columns * heads), jnp.float32),
            pltpu.VMEM((heads, rows, columns), low),
            pltpu.VMEM((hops, rows, columns), low),
            pltpu.VMEM((hops, rows, columns), low),
            pltpu.SemaphoreType.DMA((2,)),
            pltpu.SemaphoreType.DMA,
            pltpu.SemaphoreType.DMA,
            pltpu.SemaphoreType.DMA((devices, 2)),
            pltpu.SemaphoreType.DMA((devices, 2)),
            pltpu.SemaphoreType.DMA((hops, chunks)),
            pltpu.SemaphoreType.DMA((hops, chunks)),
            pltpu.SemaphoreType.DMA((hops, chunks)),
            pltpu.SemaphoreType.DMA((hops, chunks)),
        ],
        compiler_params=pltpu.CompilerParams(
            collective_id=0, has_side_effects=True, vmem_limit_bytes=62 * 1024 * 1024
        ),
    )(
        tile_counts, attn_gate, queries, image_range, image_keys, image_values, out_weight,
        layer_input,
    )


def solution(mesh):
    in_specs = (
        P("seq", "head"),
        P("seq", "head"),
        P("seq", "head"),
        P("seq", "head"),
        P("head", None),
        P(),
        P(None, "seq"),
        P(),
    )
    out_specs = P("seq", "head")
    return jax.shard_map(shards, mesh=mesh, in_specs=in_specs, out_specs=out_specs, check_vma=False)
```

```python
import functools
import math

import jax
import jax.numpy as jnp
from jax import lax
from jax.experimental import pallas as pl
from jax.experimental.pallas import tpu as pltpu
from jax.sharding import PartitionSpec as P

MESH = pl.DeviceIdType.MESH
NEG = -1e30
BIG = 1e30
LANES = 128
PACK = 16
LAG = 1


def round_up(value, unit):
    return -(-value // unit) * unit


def kernel(
    plan,
    counts_ref,
    gate_ref,
    q_ref,
    range_ref,
    k_hbm,
    v_hbm,
    w_hbm,
    x_hbm,
    out_ref,
    kv,
    staged,
    weight,
    residual,
    q_wide,
    bounds,
    scores,
    values,
    run_max,
    numer,
    turned,
    attended,
    term,
    sent,
    from_left,
    from_right,
    own_sem,
    weight_sem,
    residual_sem,
    kv_send,
    kv_recv,
    right_send,
    right_recv,
    left_send,
    left_recv,
    lent_weight,
    lent_rows,
    lent_send,
    lent_recv,
    rows_send,
    rows_recv,
):
    devices, heads, tile_rows, split, padded, images, chunks, strip = plan
    square = devices == 8
    chips = devices // 2
    me = lax.axis_index("seq")
    h = lax.axis_index("head")
    core = lax.rem(me, 2)
    chip = me // 2
    partner = chip * 2 + (1 - core)
    rows, width = q_ref.shape
    head_dim = kv.shape[3]
    group = width // head_dim
    strips = group * rows // strip
    columns = out_ref.shape[1]
    halves = ((0, split), (split, padded - split))

    def chip_at(offset):
        if square:
            cy, cx = chip // 2, lax.rem(chip, 2)
            oy, ox = offset // 2, lax.rem(offset, 2)
            return lax.rem(cy + oy, 2) * 2 + lax.rem(cx + ox, 2)
        return lax.rem(chip + offset, chips)

    def at(target):
        return (target, h)

    own = [
        pltpu.make_async_copy(
            source, staged.at[which], own_sem.at[which]
        )
        for which, source in enumerate((k_hbm, v_hbm))
    ]
    for copy in own:
        copy.start()
    fetch = pltpu.make_async_copy(w_hbm, weight, weight_sem)
    fetch.start()
    take = pltpu.make_async_copy(x_hbm, residual, residual_sem)
    take.start()

    barrier = pltpu.get_barrier_semaphore()
    pl.semaphore_signal(barrier, inc=1, device_id=at(partner), device_id_type=MESH)
    for offset in range(1, chips):
        pl.semaphore_signal(
            barrier, inc=1, device_id=at(chip_at(offset) * 2 + core), device_id_type=MESH
        )
    greeted = chips

    @pl.when(h > 0)
    def _():
        pl.semaphore_signal(barrier, inc=1, device_id=(me, h - 1), device_id_type=MESH)

    @pl.when(h < heads - 1)
    def _():
        pl.semaphore_signal(barrier, inc=1, device_id=(me, h + 1), device_id_type=MESH)

    ends = jnp.where(h > 0, 1, 0) + jnp.where(h < heads - 1, 1, 0)

    factor = math.log2(math.e) / math.sqrt(head_dim)
    run_max[...] = jnp.full_like(run_max, NEG)
    numer[...] = jnp.zeros_like(numer)
    values[...] = jnp.ones_like(values)
    for g in range(group):
        exact = q_ref[:, g * head_dim : (g + 1) * head_dim].astype(jnp.float32) * factor
        high = exact.astype(jnp.bfloat16)
        part = pl.ds(g * rows, rows)
        q_wide[:head_dim, part] = high.T
        q_wide[head_dim:, part] = (exact - high.astype(jnp.float32)).astype(jnp.bfloat16).T
        bounds[:, part] = range_ref[...]
    whole_rows = tile_rows // PACK * PACK
    for which, copy in enumerate(own):
        copy.wait()
        kv[me, which, :whole_rows, :] = staged[which, :whole_rows, :]
        if whole_rows < padded:
            rest = staged[which, whole_rows:, :]
            kv[me, which, whole_rows:, :] = jnp.concatenate(
                [rest, jnp.zeros((padded - tile_rows, head_dim), rest.dtype)], axis=0
            )
    pl.semaphore_wait(barrier, greeted + ends)

    def kv_copy(slot, half, target, lane):
        start, size = halves[half]
        piece = kv.at[slot, :, pl.ds(start, size), :]
        return pltpu.make_async_remote_copy(
            src_ref=piece,
            dst_ref=piece,
            send_sem=kv_send.at[lane, half],
            recv_sem=kv_recv.at[slot, half],
            device_id=at(target),
            device_id_type=MESH,
        )

    def outgoing(offset, half):
        return kv_copy(me, half, chip_at(offset) * 2 + core, chips + offset)

    def to_partner(offset, half):
        return kv_copy(chip_at(offset) * 2 + core, half, partner, offset)

    def relay(half):
        source = 1 if half == 0 else 2
        return kv_copy(
            chip_at(source) * 2 + core, half, chip_at(3 - source) * 2 + core, chips + 3
        )

    share = width // devices
    lends = (h == 0) | (h == heads - 1)
    borrows = (h == 1) | (h == heads - 2)
    borrower = jnp.where(h < 2, 1, heads - 2)

    def lent_piece(slot):
        return lent_weight.at[pl.ds(pl.multiple_of(slot * share, share), share), :]

    lend = pltpu.make_async_remote_copy(
        src_ref=w_hbm.at[
            pl.ds(pl.multiple_of(me * share, share), share),
            pl.ds(pl.multiple_of(borrower * columns, LANES), columns),
        ],
        dst_ref=lent_piece(me),
        send_sem=lent_send.at[0],
        recv_sem=lent_recv.at[me],
        device_id=(me, borrower),
        device_id_type=MESH,
    )

    @pl.when(lends)
    def _():
        lend.start()

    def lent_copy(slot, target, lane):
        return pltpu.make_async_remote_copy(
            src_ref=lent_piece(slot),
            dst_ref=lent_piece(slot),
            send_sem=lent_send.at[lane],
            recv_sem=lent_recv.at[slot],
            device_id=at(target),
            device_id_type=MESH,
        )

    def lent_out(offset):
        return lent_copy(me, chip_at(offset) * 2 + core, chips + offset)

    def lent_over(offset):
        return lent_copy(chip_at(offset) * 2 + core, partner, 1 + offset)

    if square:
        outgoing(1, 0).start()
        outgoing(2, 1).start()
        outgoing(1, 1).start()
        outgoing(2, 0).start()
    else:
        for offset in range(1, chips):
            for half in range(2):
                outgoing(offset, half).start()

    to_partner(0, 0).start()
    to_partner(0, 1).start()

    def image_of(slot):
        image, end = 0, 0
        for i in range(images):
            end = end + counts_ref[i]
            image = image + jnp.where(end <= slot, 1, 0)
        return image

    real = tile_rows - split
    edge = real // PACK * PACK

    def attend(slot_a, slot_b):
        image_a, image_b = image_of(slot_a), image_of(slot_b)
        values[:head_dim, :split] = kv[slot_a, 1, :split, :].T
        values[:head_dim, split:] = kv[slot_b, 1, split:, :].T

        def lanes(g):
            return slice(g * strip, (g + 1) * strip)

        def allowed(g, image):
            low, high = bounds[0:1, lanes(g)], bounds[1:2, lanes(g)]
            return (low <= image) & (image < high)

        def score(g):
            q = q_wide[:, lanes(g)]

            def one(keys):
                return jnp.dot(
                    jnp.concatenate([keys, keys], axis=1), q, preferred_element_type=jnp.float32
                )

            s_a = one(kv[slot_a, 0, :split, :])
            s_b = one(kv[slot_b, 0, split:, :])
            row = lax.broadcasted_iota(jnp.int32, s_b[edge:].shape, 0)
            s_b = jnp.concatenate([s_b[:edge], jnp.where(row < real - edge, s_b[edge:], NEG)], axis=0)
            scores[g % 2, :split, :] = s_a
            scores[g % 2, split:, :] = s_b
            return jnp.max(s_a, axis=0, keepdims=True), jnp.max(s_b, axis=0, keepdims=True)

        def mix(g, tops):
            ok_a, ok_b = allowed(g, image_a), allowed(g, image_b)
            old = run_max[g]
            new = jnp.maximum(
                old, jnp.maximum(jnp.where(ok_a, tops[0], NEG), jnp.where(ok_b, tops[1], NEG))
            )
            base_a = jnp.where(ok_a, new, BIG)
            base_b = jnp.where(ok_b, new, BIG)
            p_a = jnp.exp2(scores[g % 2, :split, :] - base_a).astype(jnp.bfloat16)
            p_b = jnp.exp2(scores[g % 2, split:, :] - base_b).astype(jnp.bfloat16)
            run_max[g] = new
            mixed = jnp.dot(
                values[...], jnp.concatenate([p_a, p_b], axis=0), preferred_element_type=jnp.float32
            )
            numer[g] = numer[g] * jnp.exp2(old - new) + mixed

        tops = score(0)
        for g in range(strips):
            later = score(g + 1) if g + 1 < strips else None
            mix(g, tops)
            tops = later

    def turn(step, carry):
        phase = step // 2
        other = lax.rem(step, 2)
        if square:
            off_a = phase
            off_b = jnp.where(phase == 1, 2, jnp.where(phase == 2, 1, phase))
        else:
            off_a = phase
            off_b = phase
        which = jnp.where(other == 0, core, 1 - core)
        slot_a = chip_at(off_a) * 2 + which
        slot_b = chip_at(off_b) * 2 + which

        @pl.when(step > 0)
        def _():
            kv_copy(slot_a, 0, partner, 0).wait_recv()
            kv_copy(slot_b, 1, partner, 0).wait_recv()

        if square:
            @pl.when(step == 2)
            def _():
                relay(0).start()
                relay(1).start()

        @pl.when((other == 0) & (step > 0))
        def _():
            to_partner(off_a, 0).start()
            to_partner(off_b, 1).start()

        attend(slot_a, slot_b)
        return carry

    lax.fori_loop(0, devices, turn, 0)

    for g in range(strips):
        part = slice(g * strip, (g + 1) * strip)
        live = bounds[0:1, part] < bounds[1:2, part]
        whole = numer[g, head_dim : head_dim + 1, :]
        result = jnp.where(live, numer[g, :head_dim, :] / jnp.where(live, whole, 1.0), 0.0)
        turned[part, :] = result.T
    for g in range(group):
        attended[:, g * head_dim : (g + 1) * head_dim] = turned[
            g * rows : (g + 1) * rows, :
        ].astype(jnp.bfloat16)
    fetch.wait()

    @pl.when(borrows)
    def _():
        lend.wait_recv()
        for offset in range(1, chips):
            lent_out(offset).start()
        lent_over(0).start()

    lend_rows = pltpu.make_async_remote_copy(
        src_ref=attended,
        dst_ref=lent_rows,
        send_sem=rows_send,
        recv_sem=rows_recv,
        device_id=(me, borrower),
        device_id_type=MESH,
    )

    piece = 512 if columns % 512 == 0 else columns
    chunk_rows = rows // chunks

    def project(dest):
        def block(j, carry):
            where = pl.ds(pl.multiple_of(dest * columns + j * piece, LANES), piece)
            term[:, where] = jnp.dot(
                attended[...], weight[:, where], preferred_element_type=jnp.float32
            )
            return carry

        lax.fori_loop(0, columns // piece, block, 0)

    def chunk_of(c):
        return pl.ds(pl.multiple_of(c * chunk_rows, chunk_rows), chunk_rows)

    def block_of(dest):
        return pl.ds(pl.multiple_of(dest * columns, LANES), columns)

    def right_copy(i, c):
        return pltpu.make_async_remote_copy(
            src_ref=sent.at[heads - 1 - i, chunk_of(c), :],
            dst_ref=from_left.at[i, chunk_of(c), :],
            send_sem=right_send.at[i, c],
            recv_sem=right_recv.at[i, c],
            device_id=(me, h + 1),
            device_id_type=MESH,
        )

    def left_copy(i, c):
        return pltpu.make_async_remote_copy(
            src_ref=sent.at[i, chunk_of(c), :],
            dst_ref=from_right.at[i, chunk_of(c), :],
            send_sem=left_send.at[i, c],
            recv_sem=left_recv.at[i, c],
            device_id=(me, h - 1),
            device_id_type=MESH,
        )

    def pass_on(dest, i, c, copy, arrived, first):
        @pl.when(first)
        def _():
            sent[dest, chunk_of(c), :] = term[chunk_of(c), block_of(dest)].astype(sent.dtype)

        @pl.when(jnp.logical_not(first))
        def _():
            copy(i, c).wait_recv()
            sent[dest, chunk_of(c), :] = (
                term[chunk_of(c), block_of(dest)]
                + arrived[i, chunk_of(c), :].astype(jnp.float32)
            ).astype(sent.dtype)

        copy(i, c).start()

    def spread(t, carry):
        to_right = t - LAG * h
        to_left = t - LAG * (heads - 1 - h)

        @pl.when(borrows & (t == (heads - 3) * chunks + LAG))
        def _():
            for offset in range(1, chips):
                lent_copy(chip_at(offset) * 2 + core, partner, 0).wait_recv()
                lent_over(offset).start()

        @pl.when((to_right >= 0) & (to_right < jnp.minimum(heads - 1 - h, heads - 2) * chunks))
        def _():
            i = to_right // chunks
            c = lax.rem(to_right, chunks)

            @pl.when(c == 0)
            def _():
                project(heads - 1 - i)

            pass_on(heads - 1 - i, i, c, right_copy, from_left, h == 0)

        @pl.when((to_left >= 0) & (to_left < jnp.minimum(h, heads - 2) * chunks))
        def _():
            i = to_left // chunks
            c = lax.rem(to_left, chunks)

            @pl.when(c == 0)
            def _():
                project(i)

            pass_on(i, i, c, left_copy, from_right, h == heads - 1)

        return carry

    lax.fori_loop(0, (heads - 2) * chunks + LAG * (heads - 1), spread, 0)

    @pl.when(lends)
    def _():
        lend_rows.start()

    project(h)

    @pl.when(borrows)
    def _():
        for offset in range(chips):
            lent_copy(chip_at(offset) * 2 + 1 - core, partner, 0).wait_recv()
        lend_rows.wait_recv()

        def block(j, carry):
            where = pl.ds(pl.multiple_of(j * piece, LANES), piece)
            into = pl.ds(pl.multiple_of(h * columns + j * piece, LANES), piece)
            term[:, into] += jnp.dot(
                lent_rows[...], lent_weight[:, where], preferred_element_type=jnp.float32
            )
            return carry

        lax.fori_loop(0, columns // piece, block, 0)

    take.wait()
    gate = jnp.tanh(jnp.full((8, LANES), gate_ref[0], jnp.float32))[0:1, 0:1]

    def gather(c, carry):
        @pl.when((h < heads - 1) & (h != heads - 2))
        def _():
            left_copy(h, c).wait_recv()
            term[chunk_of(c), block_of(h)] += from_right[h, chunk_of(c), :].astype(jnp.float32)

        @pl.when((h > 0) & (h != 1))
        def _():
            right_copy(heads - 1 - h, c).wait_recv()
            term[chunk_of(c), block_of(h)] += from_left[heads - 1 - h, chunk_of(c), :].astype(
                jnp.float32
            )

        out_ref[chunk_of(c), :] = (
            residual[chunk_of(c), :].astype(jnp.float32) + gate * term[chunk_of(c), block_of(h)]
        ).astype(out_ref.dtype)
        return carry

    lax.fori_loop(0, chunks, gather, 0)

    for offset in range(chips):
        for half in range(2):
            to_partner(offset, half).wait_send()
            if square and offset == 3:
                relay(half).wait_send()
            elif offset > 0:
                outgoing(offset, half).wait_send()

    def drain(i, carry):
        def one_chunk(c, inner):
            @pl.when(h < heads - 1 - i)
            def _():
                right_copy(i, c).wait_send()

            @pl.when(h > i)
            def _():
                left_copy(i, c).wait_send()

            return inner

        lax.fori_loop(0, chunks, one_chunk, 0)
        return carry

    lax.fori_loop(0, heads - 2, drain, 0)

    @pl.when(lends)
    def _():
        lend.wait_send()
        lend_rows.wait_send()

    @pl.when(borrows)
    def _():
        for offset in range(chips):
            lent_over(offset).wait_send()
            if offset > 0:
                lent_out(offset).wait_send()


def shards(
    queries, image_keys, image_values, layer_input, out_weight, tile_counts, image_range, attn_gate
):
    devices = lax.axis_size("seq")
    heads = lax.axis_size("head")
    rows, width = queries.shape
    tile_rows, head_dim = image_keys.shape
    group = width // head_dim
    columns = layer_input.shape[1]
    padded = round_up(tile_rows, PACK)
    split = max(round_up(padded // 2 - LANES, LANES), LANES)
    chunks = 4 if rows % (4 * PACK) == 0 else 1
    images = tile_counts.shape[0]
    strip = math.gcd(group * rows, 2 * LANES)
    strips = group * rows // strip
    plan = (devices, heads, tile_rows, split, padded, images, chunks, strip)
    low = jnp.bfloat16
    vmem = pl.BlockSpec(memory_space=pltpu.VMEM)
    smem = pl.BlockSpec(memory_space=pltpu.SMEM)
    hbm = pl.BlockSpec(memory_space=pl.ANY)
    hops = heads - 2
    return pl.pallas_call(
        functools.partial(kernel, plan),
        out_shape=jax.ShapeDtypeStruct((rows, columns), low),
        in_specs=[smem, smem, vmem, vmem, hbm, hbm, hbm, hbm],
        out_specs=vmem,
        scratch_shapes=[
            pltpu.VMEM((devices, 2, padded, head_dim), low),
            pltpu.VMEM((2, tile_rows, head_dim), low),
            pltpu.VMEM(out_weight.shape, low),
            pltpu.VMEM((rows, columns), low),
            pltpu.VMEM((2 * head_dim, group * rows), low),
            pltpu.VMEM((2, group * rows), jnp.int32),
            pltpu.VMEM((2, padded, strip), jnp.float32),
            pltpu.VMEM((head_dim + PACK, padded), low),
            pltpu.VMEM((strips, 1, strip), jnp.float32),
            pltpu.VMEM((strips, head_dim + PACK, strip), jnp.float32),
            pltpu.VMEM((group * rows, head_dim), jnp.float32),
            pltpu.VMEM((rows, width), low),
            pltpu.VMEM((rows, columns * heads), jnp.float32),
            pltpu.VMEM((heads, rows, columns), low),
            pltpu.VMEM((hops, rows, columns), low),
            pltpu.VMEM((hops, rows, columns), low),
            pltpu.SemaphoreType.DMA((2,)),
            pltpu.SemaphoreType.DMA,
            pltpu.SemaphoreType.DMA,
            pltpu.SemaphoreType.DMA((devices, 2)),
            pltpu.SemaphoreType.DMA((devices, 2)),
            pltpu.SemaphoreType.DMA((hops, chunks)),
            pltpu.SemaphoreType.DMA((hops, chunks)),
            pltpu.SemaphoreType.DMA((hops, chunks)),
            pltpu.SemaphoreType.DMA((hops, chunks)),
            pltpu.VMEM((width, columns), low),
            pltpu.VMEM((rows, width), low),
            pltpu.SemaphoreType.DMA((devices + 1,)),
            pltpu.SemaphoreType.DMA((devices,)),
            pltpu.SemaphoreType.DMA,
            pltpu.SemaphoreType.DMA,
        ],
        compiler_params=pltpu.CompilerParams(
            collective_id=0, has_side_effects=True, vmem_limit_bytes=62 * 1024 * 1024
        ),
    )(
        tile_counts, attn_gate, queries, image_range, image_keys, image_values, out_weight,
        layer_input,
    )


def solution(mesh):
    in_specs = (
        P("seq", "head"),
        P("seq", "head"),
        P("seq", "head"),
        P("seq", "head"),
        P("head", None),
        P(),
        P(None, "seq"),
        P(),
    )
    out_specs = P("seq", "head")
    return jax.shard_map(shards, mesh=mesh, in_specs=in_specs, out_specs=out_specs, check_vma=False)
```

```python
import functools
import math

import jax
import jax.numpy as jnp
from jax import lax
from jax.experimental import pallas as pl
from jax.experimental.pallas import tpu as pltpu
from jax.sharding import PartitionSpec as P

MESH = pl.DeviceIdType.MESH
NEG = -1e30
BIG = 1e30
LANES = 128
PACK = 16
LAG = 1


def round_up(value, unit):
    return -(-value // unit) * unit


def kernel(
    plan,
    counts_ref,
    gate_ref,
    q_ref,
    range_ref,
    k_hbm,
    v_hbm,
    w_hbm,
    x_hbm,
    out_ref,
    kv,
    staged,
    weight,
    residual,
    q_wide,
    bounds,
    scores,
    values,
    run_max,
    numer,
    turned,
    attended,
    term,
    sent,
    from_left,
    from_right,
    own_sem,
    weight_sem,
    residual_sem,
    kv_send,
    kv_recv,
    right_send,
    right_recv,
    left_send,
    left_recv,
    lent_weight,
    lent_rows,
    lent_send,
    lent_recv,
    rows_send,
    rows_recv,
):
    devices, heads, tile_rows, split, padded, images, chunks, strip = plan
    square = devices == 8
    chips = devices // 2
    me = lax.axis_index("seq")
    h = lax.axis_index("head")
    core = lax.rem(me, 2)
    chip = me // 2
    partner = chip * 2 + (1 - core)
    rows, width = q_ref.shape
    head_dim = kv.shape[3]
    group = width // head_dim
    strips = group * rows // strip
    columns = out_ref.shape[1]
    halves = ((0, split), (split, padded - split))

    def chip_at(offset):
        if square:
            cy, cx = chip // 2, lax.rem(chip, 2)
            oy, ox = offset // 2, lax.rem(offset, 2)
            return lax.rem(cy + oy, 2) * 2 + lax.rem(cx + ox, 2)
        return lax.rem(chip + offset, chips)

    def at(target):
        return (target, h)

    own = [
        pltpu.make_async_copy(
            source, staged.at[which], own_sem.at[which]
        )
        for which, source in enumerate((k_hbm, v_hbm))
    ]
    for copy in own:
        copy.start()
    fetch = pltpu.make_async_copy(w_hbm, weight, weight_sem)
    fetch.start()
    take = pltpu.make_async_copy(x_hbm, residual, residual_sem)
    take.start()

    barrier = pltpu.get_barrier_semaphore()
    pl.semaphore_signal(barrier, inc=1, device_id=at(partner), device_id_type=MESH)
    for offset in range(1, chips):
        pl.semaphore_signal(
            barrier, inc=1, device_id=at(chip_at(offset) * 2 + core), device_id_type=MESH
        )
    greeted = chips

    @pl.when(h > 0)
    def _():
        pl.semaphore_signal(barrier, inc=1, device_id=(me, h - 1), device_id_type=MESH)

    @pl.when(h < heads - 1)
    def _():
        pl.semaphore_signal(barrier, inc=1, device_id=(me, h + 1), device_id_type=MESH)

    ends = jnp.where(h > 0, 1, 0) + jnp.where(h < heads - 1, 1, 0)

    whole_rows = tile_rows // PACK * PACK
    for which, copy in enumerate(own):
        copy.wait()
        kv[me, which, :whole_rows, :] = staged[which, :whole_rows, :]
        if whole_rows < padded:
            rest = staged[which, whole_rows:, :]
            kv[me, which, whole_rows:, :] = jnp.concatenate(
                [rest, jnp.zeros((padded - tile_rows, head_dim), rest.dtype)], axis=0
            )
    pl.semaphore_wait(barrier, greeted + ends)

    def kv_copy(slot, half, target, lane):
        start, size = halves[half]
        piece = kv.at[slot, :, pl.ds(start, size), :]
        return pltpu.make_async_remote_copy(
            src_ref=piece,
            dst_ref=piece,
            send_sem=kv_send.at[lane, half],
            recv_sem=kv_recv.at[slot, half],
            device_id=at(target),
            device_id_type=MESH,
        )

    def outgoing(offset, half):
        return kv_copy(me, half, chip_at(offset) * 2 + core, chips + offset)

    def to_partner(offset, half):
        return kv_copy(chip_at(offset) * 2 + core, half, partner, offset)

    def relay(half):
        source = 1 if half == 0 else 2
        return kv_copy(
            chip_at(source) * 2 + core, half, chip_at(3 - source) * 2 + core, chips + 3
        )

    share = width // devices
    lends = (h == 0) | (h == heads - 1)
    borrows = (h == 1) | (h == heads - 2)
    borrower = jnp.where(h < 2, 1, heads - 2)

    def lent_piece(slot):
        return lent_weight.at[pl.ds(pl.multiple_of(slot * share, share), share), :]

    lend = pltpu.make_async_remote_copy(
        src_ref=w_hbm.at[
            pl.ds(pl.multiple_of(me * share, share), share),
            pl.ds(pl.multiple_of(borrower * columns, LANES), columns),
        ],
        dst_ref=lent_piece(me),
        send_sem=lent_send.at[0],
        recv_sem=lent_recv.at[me],
        device_id=(me, borrower),
        device_id_type=MESH,
    )

    @pl.when(lends)
    def _():
        lend.start()

    def lent_copy(slot, target, lane):
        return pltpu.make_async_remote_copy(
            src_ref=lent_piece(slot),
            dst_ref=lent_piece(slot),
            send_sem=lent_send.at[lane],
            recv_sem=lent_recv.at[slot],
            device_id=at(target),
            device_id_type=MESH,
        )

    def lent_out(offset):
        return lent_copy(me, chip_at(offset) * 2 + core, chips + offset)

    def lent_over(offset):
        return lent_copy(chip_at(offset) * 2 + core, partner, 1 + offset)

    if square:
        outgoing(1, 0).start()
        outgoing(2, 1).start()
        outgoing(1, 1).start()
        outgoing(2, 0).start()
    else:
        for offset in range(1, chips):
            for half in range(2):
                outgoing(offset, half).start()

    to_partner(0, 0).start()
    to_partner(0, 1).start()

    factor = math.log2(math.e) / math.sqrt(head_dim)
    run_max[...] = jnp.full_like(run_max, NEG)
    numer[...] = jnp.zeros_like(numer)
    values[...] = jnp.ones_like(values)
    for g in range(group):
        exact = q_ref[:, g * head_dim : (g + 1) * head_dim].astype(jnp.float32) * factor
        high = exact.astype(jnp.bfloat16)
        part = pl.ds(g * rows, rows)
        q_wide[:head_dim, part] = high.T
        q_wide[head_dim:, part] = (exact - high.astype(jnp.float32)).astype(jnp.bfloat16).T
        bounds[:, part] = range_ref[...]

    def image_of(slot):
        image, end = 0, 0
        for i in range(images):
            end = end + counts_ref[i]
            image = image + jnp.where(end <= slot, 1, 0)
        return image

    real = tile_rows - split
    edge = real // PACK * PACK

    def attend(slot_a, slot_b):
        image_a, image_b = image_of(slot_a), image_of(slot_b)
        values[:head_dim, :split] = kv[slot_a, 1, :split, :].T
        values[:head_dim, split:] = kv[slot_b, 1, split:, :].T

        def lanes(g):
            return slice(g * strip, (g + 1) * strip)

        def allowed(g, image):
            low, high = bounds[0:1, lanes(g)], bounds[1:2, lanes(g)]
            return (low <= image) & (image < high)

        def score(g):
            q = q_wide[:, lanes(g)]

            def one(keys):
                return jnp.dot(
                    jnp.concatenate([keys, keys], axis=1), q, preferred_element_type=jnp.float32
                )

            s_a = one(kv[slot_a, 0, :split, :])
            s_b = one(kv[slot_b, 0, split:, :])
            row = lax.broadcasted_iota(jnp.int32, s_b[edge:].shape, 0)
            s_b = jnp.concatenate([s_b[:edge], jnp.where(row < real - edge, s_b[edge:], NEG)], axis=0)
            scores[g % 2, :split, :] = s_a
            scores[g % 2, split:, :] = s_b
            return jnp.max(s_a, axis=0, keepdims=True), jnp.max(s_b, axis=0, keepdims=True)

        def mix(g, tops):
            ok_a, ok_b = allowed(g, image_a), allowed(g, image_b)
            old = run_max[g]
            new = jnp.maximum(
                old, jnp.maximum(jnp.where(ok_a, tops[0], NEG), jnp.where(ok_b, tops[1], NEG))
            )
            base_a = jnp.where(ok_a, new, BIG)
            base_b = jnp.where(ok_b, new, BIG)
            p_a = jnp.exp2(scores[g % 2, :split, :] - base_a).astype(jnp.bfloat16)
            p_b = jnp.exp2(scores[g % 2, split:, :] - base_b).astype(jnp.bfloat16)
            run_max[g] = new
            mixed = jnp.dot(
                values[...], jnp.concatenate([p_a, p_b], axis=0), preferred_element_type=jnp.float32
            )
            numer[g] = numer[g] * jnp.exp2(old - new) + mixed

        tops = score(0)
        for g in range(strips):
            later = score(g + 1) if g + 1 < strips else None
            mix(g, tops)
            tops = later

    def turn(step, carry):
        phase = step // 2
        other = lax.rem(step, 2)
        if square:
            off_a = phase
            off_b = jnp.where(phase == 1, 2, jnp.where(phase == 2, 1, phase))
        else:
            off_a = phase
            off_b = phase
        which = jnp.where(other == 0, core, 1 - core)
        slot_a = chip_at(off_a) * 2 + which
        slot_b = chip_at(off_b) * 2 + which

        @pl.when(step > 0)
        def _():
            kv_copy(slot_a, 0, partner, 0).wait_recv()
            kv_copy(slot_b, 1, partner, 0).wait_recv()

        if square:
            @pl.when(step == 2)
            def _():
                relay(0).start()
                relay(1).start()

        @pl.when((other == 0) & (step > 0))
        def _():
            to_partner(off_a, 0).start()
            to_partner(off_b, 1).start()

        attend(slot_a, slot_b)
        return carry

    lax.fori_loop(0, devices, turn, 0)

    for g in range(strips):
        part = slice(g * strip, (g + 1) * strip)
        live = bounds[0:1, part] < bounds[1:2, part]
        whole = numer[g, head_dim : head_dim + 1, :]
        result = jnp.where(live, numer[g, :head_dim, :] / jnp.where(live, whole, 1.0), 0.0)
        turned[part, :] = result.T
    for g in range(group):
        attended[:, g * head_dim : (g + 1) * head_dim] = turned[
            g * rows : (g + 1) * rows, :
        ].astype(jnp.bfloat16)
    fetch.wait()

    @pl.when(borrows)
    def _():
        lend.wait_recv()
        for offset in range(1, chips):
            lent_out(offset).start()
        lent_over(0).start()

    lend_rows = pltpu.make_async_remote_copy(
        src_ref=attended,
        dst_ref=lent_rows,
        send_sem=rows_send,
        recv_sem=rows_recv,
        device_id=(me, borrower),
        device_id_type=MESH,
    )

    piece = 512 if columns % 512 == 0 else columns
    chunk_rows = rows // chunks

    def project(dest):
        def block(j, carry):
            where = pl.ds(pl.multiple_of(dest * columns + j * piece, LANES), piece)
            term[:, where] = jnp.dot(
                attended[...], weight[:, where], preferred_element_type=jnp.float32
            )
            return carry

        lax.fori_loop(0, columns // piece, block, 0)

    def chunk_of(c):
        return pl.ds(pl.multiple_of(c * chunk_rows, chunk_rows), chunk_rows)

    def block_of(dest):
        return pl.ds(pl.multiple_of(dest * columns, LANES), columns)

    def right_copy(i, c):
        return pltpu.make_async_remote_copy(
            src_ref=sent.at[heads - 1 - i, chunk_of(c), :],
            dst_ref=from_left.at[i, chunk_of(c), :],
            send_sem=right_send.at[i, c],
            recv_sem=right_recv.at[i, c],
            device_id=(me, h + 1),
            device_id_type=MESH,
        )

    def left_copy(i, c):
        return pltpu.make_async_remote_copy(
            src_ref=sent.at[i, chunk_of(c), :],
            dst_ref=from_right.at[i, chunk_of(c), :],
            send_sem=left_send.at[i, c],
            recv_sem=left_recv.at[i, c],
            device_id=(me, h - 1),
            device_id_type=MESH,
        )

    def pass_on(dest, i, c, copy, arrived, first):
        @pl.when(first)
        def _():
            sent[dest, chunk_of(c), :] = term[chunk_of(c), block_of(dest)].astype(sent.dtype)

        @pl.when(jnp.logical_not(first))
        def _():
            copy(i, c).wait_recv()
            sent[dest, chunk_of(c), :] = (
                term[chunk_of(c), block_of(dest)]
                + arrived[i, chunk_of(c), :].astype(jnp.float32)
            ).astype(sent.dtype)

        copy(i, c).start()

    def spread(t, carry):
        to_right = t - LAG * h
        to_left = t - LAG * (heads - 1 - h)

        @pl.when(borrows & (t == (heads - 3) * chunks + LAG))
        def _():
            for offset in range(1, chips):
                lent_copy(chip_at(offset) * 2 + core, partner, 0).wait_recv()
                lent_over(offset).start()

        @pl.when((to_right >= 0) & (to_right < jnp.minimum(heads - 1 - h, heads - 2) * chunks))
        def _():
            i = to_right // chunks
            c = lax.rem(to_right, chunks)

            @pl.when(c == 0)
            def _():
                project(heads - 1 - i)

            pass_on(heads - 1 - i, i, c, right_copy, from_left, h == 0)

        @pl.when((to_left >= 0) & (to_left < jnp.minimum(h, heads - 2) * chunks))
        def _():
            i = to_left // chunks
            c = lax.rem(to_left, chunks)

            @pl.when(c == 0)
            def _():
                project(i)

            pass_on(i, i, c, left_copy, from_right, h == heads - 1)

        return carry

    lax.fori_loop(0, (heads - 2) * chunks + LAG * (heads - 1), spread, 0)

    @pl.when(lends)
    def _():
        lend_rows.start()

    project(h)

    @pl.when(borrows)
    def _():
        for offset in range(chips):
            lent_copy(chip_at(offset) * 2 + 1 - core, partner, 0).wait_recv()
        lend_rows.wait_recv()

        def block(j, carry):
            where = pl.ds(pl.multiple_of(j * piece, LANES), piece)
            into = pl.ds(pl.multiple_of(h * columns + j * piece, LANES), piece)
            term[:, into] += jnp.dot(
                lent_rows[...], lent_weight[:, where], preferred_element_type=jnp.float32
            )
            return carry

        lax.fori_loop(0, columns // piece, block, 0)

    take.wait()
    gate = jnp.tanh(jnp.full((8, LANES), gate_ref[0], jnp.float32))[0:1, 0:1]

    def gather(c, carry):
        @pl.when((h < heads - 1) & (h != heads - 2))
        def _():
            left_copy(h, c).wait_recv()
            term[chunk_of(c), block_of(h)] += from_right[h, chunk_of(c), :].astype(jnp.float32)

        @pl.when((h > 0) & (h != 1))
        def _():
            right_copy(heads - 1 - h, c).wait_recv()
            term[chunk_of(c), block_of(h)] += from_left[heads - 1 - h, chunk_of(c), :].astype(
                jnp.float32
            )

        out_ref[chunk_of(c), :] = (
            residual[chunk_of(c), :].astype(jnp.float32) + gate * term[chunk_of(c), block_of(h)]
        ).astype(out_ref.dtype)
        return carry

    lax.fori_loop(0, chunks, gather, 0)

    for offset in range(chips):
        for half in range(2):
            to_partner(offset, half).wait_send()
            if square and offset == 3:
                relay(half).wait_send()
            elif offset > 0:
                outgoing(offset, half).wait_send()

    def drain(i, carry):
        def one_chunk(c, inner):
            @pl.when(h < heads - 1 - i)
            def _():
                right_copy(i, c).wait_send()

            @pl.when(h > i)
            def _():
                left_copy(i, c).wait_send()

            return inner

        lax.fori_loop(0, chunks, one_chunk, 0)
        return carry

    lax.fori_loop(0, heads - 2, drain, 0)

    @pl.when(lends)
    def _():
        lend.wait_send()
        lend_rows.wait_send()

    @pl.when(borrows)
    def _():
        for offset in range(chips):
            lent_over(offset).wait_send()
            if offset > 0:
                lent_out(offset).wait_send()


def shards(
    queries, image_keys, image_values, layer_input, out_weight, tile_counts, image_range, attn_gate
):
    devices = lax.axis_size("seq")
    heads = lax.axis_size("head")
    rows, width = queries.shape
    tile_rows, head_dim = image_keys.shape
    group = width // head_dim
    columns = layer_input.shape[1]
    padded = round_up(tile_rows, PACK)
    split = max(round_up(padded // 2 - LANES, LANES), LANES)
    chunks = 4 if rows % (4 * PACK) == 0 else 1
    images = tile_counts.shape[0]
    strip = math.gcd(group * rows, 2 * LANES)
    strips = group * rows // strip
    plan = (devices, heads, tile_rows, split, padded, images, chunks, strip)
    low = jnp.bfloat16
    vmem = pl.BlockSpec(memory_space=pltpu.VMEM)
    smem = pl.BlockSpec(memory_space=pltpu.SMEM)
    hbm = pl.BlockSpec(memory_space=pl.ANY)
    hops = heads - 2
    return pl.pallas_call(
        functools.partial(kernel, plan),
        out_shape=jax.ShapeDtypeStruct((rows, columns), low),
        in_specs=[smem, smem, vmem, vmem, hbm, hbm, hbm, hbm],
        out_specs=vmem,
        scratch_shapes=[
            pltpu.VMEM((devices, 2, padded, head_dim), low),
            pltpu.VMEM((2, tile_rows, head_dim), low),
            pltpu.VMEM(out_weight.shape, low),
            pltpu.VMEM((rows, columns), low),
            pltpu.VMEM((2 * head_dim, group * rows), low),
            pltpu.VMEM((2, group * rows), jnp.int32),
            pltpu.VMEM((2, padded, strip), jnp.float32),
            pltpu.VMEM((head_dim + PACK, padded), low),
            pltpu.VMEM((strips, 1, strip), jnp.float32),
            pltpu.VMEM((strips, head_dim + PACK, strip), jnp.float32),
            pltpu.VMEM((group * rows, head_dim), jnp.float32),
            pltpu.VMEM((rows, width), low),
            pltpu.VMEM((rows, columns * heads), jnp.float32),
            pltpu.VMEM((heads, rows, columns), low),
            pltpu.VMEM((hops, rows, columns), low),
            pltpu.VMEM((hops, rows, columns), low),
            pltpu.SemaphoreType.DMA((2,)),
            pltpu.SemaphoreType.DMA,
            pltpu.SemaphoreType.DMA,
            pltpu.SemaphoreType.DMA((devices, 2)),
            pltpu.SemaphoreType.DMA((devices, 2)),
            pltpu.SemaphoreType.DMA((hops, chunks)),
            pltpu.SemaphoreType.DMA((hops, chunks)),
            pltpu.SemaphoreType.DMA((hops, chunks)),
            pltpu.SemaphoreType.DMA((hops, chunks)),
            pltpu.VMEM((width, columns), low),
            pltpu.VMEM((rows, width), low),
            pltpu.SemaphoreType.DMA((devices + 1,)),
            pltpu.SemaphoreType.DMA((devices,)),
            pltpu.SemaphoreType.DMA,
            pltpu.SemaphoreType.DMA,
        ],
        compiler_params=pltpu.CompilerParams(
            collective_id=0, has_side_effects=True, vmem_limit_bytes=62 * 1024 * 1024
        ),
    )(
        tile_counts, attn_gate, queries, image_range, image_keys, image_values, out_weight,
        layer_input,
    )


def solution(mesh):
    in_specs = (
        P("seq", "head"),
        P("seq", "head"),
        P("seq", "head"),
        P("seq", "head"),
        P("head", None),
        P(),
        P(None, "seq"),
        P(),
    )
    out_specs = P("seq", "head")
    return jax.shard_map(shards, mesh=mesh, in_specs=in_specs, out_specs=out_specs, check_vma=False)
```
